64 devices in a mesh: req: 4 (over x, y), cp: 16 (over z, core).
Axes of the slice: x: 2, y: 2, z: 8, core: 2. Of those that a mesh axis runs over, the one named last changes fastest.
The devices are a block of a 4x4x8 slice.
Arguments:
- hidden: bfloat16 [4096, 2048], P(('req', 'cp')), parts along dimension 0
- positions: int32 [4096], P(('req', 'cp')), parts along dimension 0
- gain_attn: bfloat16 [3, 2048], replicated
- gain_mlp: bfloat16 [3, 2048], replicated
- w_query: bfloat16 [3, 2048, 16, 128], replicated
- w_key: bfloat16 [3, 2048, 16, 128], replicated
- w_value: bfloat16 [3, 2048, 16, 128], replicated
- w_out: bfloat16 [3, 16, 128, 2048], replicated
- w_gate: bfloat16 [3, 2048, 5504], replicated
- w_up: bfloat16 [3, 2048, 5504], replicated
- w_down: bfloat16 [3, 5504, 2048], replicated
Outputs:
- output 1: bfloat16 [4096, 2048], P(('req', 'cp')), parts along dimension 0
- output 2: bfloat16 [3, 4096, 16, 128], P(None, 'req', 'cp'), parts along dimension 1
- output 3: bfloat16 [3, 4096, 16, 128], P(None, 'req', 'cp'), parts along dimension 1
There are 4 independent parts. The reference program is written for one: setup_inputs(seed, part) draws one part's arguments, and reference() takes and returns one part's arrays. A program takes and returns all parts, laid end to end along the dimension named above; an argument that names none is the same for every part.
All inputs are finite; a program needn't handle non-finite values.
Results may differ from the reference program's by a relative error of at most 0.02.
Values are sent between devices in bfloat16 or wider.
A program may use at most 768 MiB of HBM per device.

```python
import jax
import jax.numpy as jnp
from jax import lax

MODEL_DIM = 2048
NUM_HEADS = 16
KV_HEADS = 16
HEAD_DIM = 128
FFN_DIM = 5504
NUM_LAYERS = 3
TOKENS_DEV = 64
CP_SIZE = 16

SEQ_LEN = CP_SIZE * TOKENS_DEV
CHUNK_LEN = TOKENS_DEV // 2
GROUP_SIZE = NUM_HEADS // KV_HEADS
NORM_EPS = 1e-5
ROPE_BASE = 10000.0


def draw_positions(pos_key):
    step_sizes = jax.random.randint(pos_key, (SEQ_LEN,), 1, 4, dtype=jnp.int32)
    natural = (jnp.cumsum(step_sizes) - step_sizes[0]).astype(jnp.int32)
    halves = natural.reshape(2, CP_SIZE, CHUNK_LEN)
    return jnp.stack([halves[0], halves[1][::-1]], axis=1).reshape(SEQ_LEN)


def setup_inputs(seed: int = 0, part: int = 0) -> dict:
    base_key = jax.random.key(seed)
    part_key = jax.random.fold_in(base_key, part)
    hidden_key, pos_key = jax.random.split(part_key, 2)
    weight_keys = jax.random.split(base_key, 9)
    dim_scale = MODEL_DIM ** -0.5
    shape_q = (NUM_LAYERS, MODEL_DIM, NUM_HEADS, HEAD_DIM)
    shape_kv = (NUM_LAYERS, MODEL_DIM, KV_HEADS, HEAD_DIM)
    shape_ff = (NUM_LAYERS, MODEL_DIM, FFN_DIM)
    shape_gain = (NUM_LAYERS, MODEL_DIM)
    hidden = jax.random.normal(hidden_key, (SEQ_LEN, MODEL_DIM), jnp.float32)
    gain_attn = 1.0 + 0.3 * jax.random.normal(weight_keys[0], shape_gain, jnp.float32)
    gain_mlp = 1.0 + 0.3 * jax.random.normal(weight_keys[1], shape_gain, jnp.float32)
    w_query = 1.5 * dim_scale * jax.random.normal(weight_keys[2], shape_q, jnp.float32)
    w_key = 1.5 * dim_scale * jax.random.normal(weight_keys[3], shape_kv, jnp.float32)
    w_value = dim_scale * jax.random.normal(weight_keys[4], shape_kv, jnp.float32)
    w_out = (NUM_HEADS * HEAD_DIM) ** -0.5 * jax.random.normal(weight_keys[5], (NUM_LAYERS, NUM_HEADS, HEAD_DIM, MODEL_DIM), jnp.float32)
    w_gate = dim_scale * jax.random.normal(weight_keys[6], shape_ff, jnp.float32)
    w_up = dim_scale * jax.random.normal(weight_keys[7], shape_ff, jnp.float32)
    w_down = FFN_DIM ** -0.5 * jax.random.normal(weight_keys[8], (NUM_LAYERS, FFN_DIM, MODEL_DIM), jnp.float32)
    return {
        "hidden": hidden.astype(jnp.bfloat16),
        "positions": draw_positions(pos_key),
        "gain_attn": gain_attn.astype(jnp.bfloat16),
        "gain_mlp": gain_mlp.astype(jnp.bfloat16),
        "w_query": w_query.astype(jnp.bfloat16),
        "w_key": w_key.astype(jnp.bfloat16),
        "w_value": w_value.astype(jnp.bfloat16),
        "w_out": w_out.astype(jnp.bfloat16),
        "w_gate": w_gate.astype(jnp.bfloat16),
        "w_up": w_up.astype(jnp.bfloat16),
        "w_down": w_down.astype(jnp.bfloat16),
    }


def rms_norm(values, gain_vec):
    wide_vals = values.astype(jnp.float32)
    inv_rms = lax.rsqrt(jnp.mean(wide_vals * wide_vals, axis=-1, keepdims=True) + NORM_EPS)
    return (wide_vals * inv_rms * gain_vec.astype(jnp.float32)).astype(jnp.bfloat16)


def rope_tables(pos_vec, head_dim):
    inv_freq = ROPE_BASE ** (-jnp.arange(0, head_dim, 2, dtype=jnp.float32) / head_dim)
    angles = pos_vec.astype(jnp.float32)[..., None] * inv_freq
    return jnp.cos(angles)[..., None, :], jnp.sin(angles)[..., None, :]


def rotate_half(values, cos_tab, sin_tab):
    half_dim = values.shape[-1] // 2
    lower_half = values[..., :half_dim]
    upper_half = values[..., half_dim:]
    return jnp.concatenate([lower_half * cos_tab - upper_half * sin_tab, upper_half * cos_tab + lower_half * sin_tab], axis=-1)


def to_natural(rows):
    split_rows = rows.reshape((CP_SIZE, 2, CHUNK_LEN) + rows.shape[1:])
    return jnp.concatenate([split_rows[:, 0], split_rows[::-1, 1]], axis=0).reshape(rows.shape)


def decoder_layer(hidden, layer_weights, cos_tab, sin_tab, positions):
    gain_attn, gain_mlp, w_query, w_key, w_value, w_out, w_gate, w_up, w_down = layer_weights
    normed = rms_norm(hidden, gain_attn)
    q_proj = jnp.dot(normed, w_query.reshape(MODEL_DIM, NUM_HEADS * HEAD_DIM), preferred_element_type=jnp.float32)
    queries = rotate_half(q_proj.reshape(SEQ_LEN, NUM_HEADS, HEAD_DIM), cos_tab, sin_tab).astype(jnp.bfloat16)
    k_proj = jnp.dot(normed, w_key.reshape(MODEL_DIM, KV_HEADS * HEAD_DIM), preferred_element_type=jnp.float32)
    key_rot = rotate_half(k_proj.reshape(SEQ_LEN, KV_HEADS, HEAD_DIM), cos_tab, sin_tab).astype(jnp.bfloat16)
    v_proj = jnp.dot(normed, w_value.reshape(MODEL_DIM, KV_HEADS * HEAD_DIM), preferred_element_type=jnp.float32)
    value_proj = v_proj.astype(jnp.bfloat16).reshape(SEQ_LEN, KV_HEADS, HEAD_DIM)
    key_wide = key_rot.astype(jnp.float32)
    value_wide = value_proj.astype(jnp.float32)
    q_blocks = queries.reshape(CP_SIZE, TOKENS_DEV, KV_HEADS, GROUP_SIZE, HEAD_DIM)
    pos_blocks = positions.reshape(CP_SIZE, TOKENS_DEV)

    def attend_block(block_in):
        q_block, pos_block = block_in
        scores = jnp.einsum("tkgd,skd->kgts", q_block.astype(jnp.float32), key_wide) * (HEAD_DIM ** -0.5)
        allowed = positions[None, :] <= pos_block[:, None]
        scores = jnp.where(allowed, scores, -jnp.inf)
        row_max = jnp.max(scores, axis=-1, keepdims=True)
        exp_scores = jnp.exp(scores - row_max)
        attn_probs = (exp_scores / jnp.sum(exp_scores, axis=-1, keepdims=True)).astype(jnp.bfloat16)
        return jnp.einsum("kgts,skd->tkgd", attn_probs.astype(jnp.float32), value_wide).astype(jnp.bfloat16)

    attn_out = lax.map(attend_block, (q_blocks, pos_blocks)).reshape(SEQ_LEN, NUM_HEADS * HEAD_DIM)
    attn_proj = jnp.dot(attn_out, w_out.reshape(NUM_HEADS * HEAD_DIM, MODEL_DIM), preferred_element_type=jnp.float32)
    hidden = (hidden.astype(jnp.float32) + attn_proj).astype(jnp.bfloat16)
    normed_mlp = rms_norm(hidden, gain_mlp)
    gate_act = jnp.dot(normed_mlp, w_gate, preferred_element_type=jnp.float32)
    up_act = jnp.dot(normed_mlp, w_up, preferred_element_type=jnp.float32)
    mlp_hidden = (jax.nn.silu(gate_act) * up_act).astype(jnp.bfloat16)
    mlp_out = jnp.dot(mlp_hidden, w_down, preferred_element_type=jnp.float32)
    hidden = (hidden.astype(jnp.float32) + mlp_out).astype(jnp.bfloat16)
    return hidden, key_rot, value_proj


def reference(hidden, positions, gain_attn, gain_mlp, w_query, w_key, w_value, w_out, w_gate, w_up, w_down):
    cos_tab, sin_tab = rope_tables(positions, HEAD_DIM)

    def layer_step(carry_hidden, layer_weights):
        new_hidden, key_rot, value_proj = decoder_layer(carry_hidden, layer_weights, cos_tab, sin_tab, positions)
        return new_hidden, (to_natural(key_rot), to_natural(value_proj))

    stacked = (gain_attn, gain_mlp, w_query, w_key, w_value, w_out, w_gate, w_up, w_down)
    final_hidden, caches = lax.scan(layer_step, hidden, stacked)
    k_cache, v_cache = caches
    return final_hidden, k_cache, v_cache
```

```python
import functools

import jax
import jax.numpy as jnp
from jax import lax
from jax.experimental import pallas as pl
from jax.experimental.pallas import tpu as pltpu
from jax.sharding import PartitionSpec as P

NORM_EPS = 1e-5
ROPE_BASE = 10000.0
F32 = jnp.float32
BF16 = jnp.bfloat16


def rope_tables(pos_vec, head_dim):
    inv_freq = ROPE_BASE ** (-jnp.arange(0, head_dim, 2, dtype=F32) / head_dim)
    angles = pos_vec.astype(F32)[..., None] * inv_freq
    cos_tab, sin_tab = jnp.cos(angles), jnp.sin(angles)
    return jnp.stack([jnp.concatenate([cos_tab, cos_tab], -1), jnp.concatenate([-sin_tab, sin_tab], -1)])


def dot(a, b):
    return jnp.dot(a, b, preferred_element_type=F32)


def kernel(cfg, x_in, cs_in, ga, gm, wq, wk, wv, wo, wg, wu, wd, x_out, kc, vc,
           xs, tab, ha, hb, acc, stage, nat, onat, orecv, act, pfull, precv, lg,
           bqkv, bo, bg, bu, bd, wsem, csem, tsend, trecv, hsend, hrecv, psend, precvs,
           qsend, qrecv, osend, orecvs):
    cp, n_layers, half, seq, heads, hd, dim, fw, foff = cfg
    seg = 2 * half
    nseg = seq // seg
    hpc = heads // 2
    me = lax.axis_index("cp")
    core = lax.rem(me, 2)
    chip = me // 2
    partner = me + 1 - 2 * core

    def al(v, m):
        return pl.multiple_of(v, m)

    my_rows = (al(half * core, half), al(seg + half * (1 - core), half))
    pa_rows = (al(half * (1 - core), half), al(seg + half * core, half))
    hbase = al(hpc * core, hpc)

    def rcopy(src, dst, ss, rs, dev):
        return pltpu.make_async_remote_copy(src_ref=src, dst_ref=dst, send_sem=ss, recv_sem=rs,
                                            device_id={"cp": dev}, device_id_type=pl.DeviceIdType.MESH)

    qkv_hbm = (wk, wq, wv)

    def w_copy(l, i):
        fo = al(core * foff, 128)
        if i < 3:
            src, dst = qkv_hbm[i].at[l, :, pl.ds(hbase, hpc), :], bqkv.at[i]
        elif i == 3:
            src, dst = wo.at[l, pl.ds(hbase, hpc)], bo
        elif i < 6:
            src, dst = (wg, wu)[i - 4].at[l, :, pl.ds(fo, fw)], (bg, bu)[i - 4]
        else:
            src, dst = wd.at[l, pl.ds(fo, fw), :], bd
        return pltpu.make_async_copy(src, dst, wsem.at[i])

    for i in range(7):
        w_copy(0, i).start()

    barrier = pltpu.get_barrier_semaphore()
    for d in range(1, cp):
        pl.semaphore_signal(barrier, inc=1, device_id={"cp": lax.rem(me + d, cp)}, device_id_type=pl.DeviceIdType.MESH)
    pl.semaphore_wait(barrier, cp - 1)

    tcp = [rcopy(cs_in.at[:, pl.ds(half * i, half), :], tab.at[:, pl.ds(my_rows[i], half), :], tsend.at[i], trecv.at[i], partner)
           for i in range(2)]
    for c in tcp:
        c.start()
    for i in range(2):
        for r in range(2):
            tab[r, pl.ds(my_rows[i], half), :] = cs_in[r, half * i:half * (i + 1), :]
    xs[...] = x_in[...].astype(F32)

    def norm_exchange(gain, hbuf):
        xv = xs[...]
        inv = lax.rsqrt(jnp.mean(xv * xv, axis=-1, keepdims=True) + NORM_EPS)
        hv = (xv * inv * gain.astype(F32)).astype(BF16)
        for i in range(2):
            hbuf[pl.ds(my_rows[i], half), :] = hv[half * i:half * (i + 1)]
        cps = [rcopy(hbuf.at[pl.ds(my_rows[i], half), :], hbuf.at[pl.ds(my_rows[i], half), :], hsend.at[i], hrecv.at[i], partner)
               for i in range(2)]
        for c in cps:
            c.start()
        for i in range(2):
            rcopy(hbuf.at[pl.ds(pa_rows[i], half), :], hbuf.at[pl.ds(pa_rows[i], half), :], hsend.at[i], hrecv.at[i], partner).wait_recv()
        for c in cps:
            c.wait_send()

    ncol = dim // 4

    def partial_exchange(product):
        def body(i, _):
            cols = pl.ds(al(i * ncol, ncol), ncol)
            pfull[:, cols] = product(cols)
            for r in range(2):
                rcopy(pfull.at[pl.ds(pa_rows[r], half), cols], precv.at[pl.ds(half * r, half), cols],
                      psend.at[i, r], precvs.at[i, r], partner).start()
            return 0
        lax.fori_loop(0, 4, body, 0)

        def done(i, _):
            cols = pl.ds(al(i * ncol, ncol), ncol)
            for r in range(2):
                rcopy(pfull.at[pl.ds(pa_rows[r], half), cols], precv.at[pl.ds(half * r, half), cols],
                      psend.at[i, r], precvs.at[i, r], partner).wait()
            for r in range(2):
                rows = slice(half * r, half * (r + 1))
                s = pfull[pl.ds(my_rows[r], half), cols] + precv[rows, cols]
                xs[rows, cols] = (xs[rows, cols] + s).astype(BF16).astype(F32)
            return 0
        lax.fori_loop(0, 4, done, 0)

    src_core = me // hpc
    my_col = lax.rem(me, hpc)

    def layer(l, _):
        par = lax.rem(l, 2)
        more = l + 1 < n_layers

        def prefetch(i):
            @pl.when(more)
            def _():
                w_copy(l + 1, i).start()

        norm_exchange(ga[l], ha)

        @pl.when(l == 0)
        def _():
            for i in range(2):
                rcopy(cs_in.at[:, pl.ds(half * i, half), :], tab.at[:, pl.ds(pa_rows[i], half), :],
                      tsend.at[i], trecv.at[i], partner).wait()

        for t in range(3):
            w_copy(l, t).wait()
            acc[...] = dot(ha[...], bqkv[t].reshape(dim, hpc * hd))
            prefetch(t)
            for j in range(hpc):
                a = acc[:, hd * j:hd * (j + 1)]
                if t < 2:
                    a = a * tab[0] + pltpu.roll(a, hd // 2, 1) * tab[1]
                stage[t, j] = a.astype(BF16)
            for j in range(hpc):
                n = hbase + j
                segs = (chip, nseg - 1 - chip)

                @pl.when(n != me)
                def _():
                    for r in range(2):
                        rcopy(stage.at[t, j, pl.ds(seg * r, seg), :], nat.at[par, t, pl.ds(al(segs[r] * seg, seg), seg), :],
                              qsend.at[t, j, r], qrecv.at[par, t, segs[r]], n).start()

                @pl.when(n == me)
                def _():
                    for r in range(2):
                        nat[par, t, pl.ds(al(segs[r] * seg, seg), seg), :] = stage[t, j, seg * r:seg * (r + 1), :]

        def wait_nat(t):
            for s in range(nseg):
                src = 2 * min(s, nseg - 1 - s) + src_core

                @pl.when(src != me)
                def _():
                    rcopy(stage.at[t, 0, pl.ds(0, seg), :], nat.at[par, t, pl.ds(s * seg, seg), :],
                          qsend.at[t, 0, 0], qrecv.at[par, t, s], src).wait_recv()

        def cache_copy(i):
            return pltpu.make_async_copy(nat.at[par, 2 * i], (kc, vc)[i].at[l], csem.at[i])

        wait_nat(0)
        cache_copy(0).start()
        wait_nat(1)
        wait_nat(2)
        cache_copy(1).start()

        qb = 256
        for b in range(seq // qb):
            n_keys = qb * (b + 1)
            q = nat[par, 1, pl.ds(qb * b, qb), :]
            k = nat[par, 0, pl.ds(0, n_keys), :]
            s = lax.dot_general(q, k, (((1,), (1,)), ((), ())), preferred_element_type=F32) * (hd ** -0.5)
            rows = lax.broadcasted_iota(jnp.int32, (qb, n_keys), 0) + qb * b
            cols = lax.broadcasted_iota(jnp.int32, (qb, n_keys), 1)
            s = jnp.where(cols <= rows, s, -jnp.inf)
            e = jnp.exp(s - jnp.max(s, axis=-1, keepdims=True))
            p = (e / jnp.sum(e, axis=-1, keepdims=True)).astype(BF16)
            onat[pl.ds(qb * b, qb), :] = dot(p, nat[par, 2, pl.ds(0, n_keys), :]).astype(BF16)
            for s_i in range(b * qb // seg, (b + 1) * qb // seg):
                r = 1 if s_i >= nseg // 2 else 0
                dest = 2 * min(s_i, nseg - 1 - s_i) + src_core
                cols_o = pl.ds(al(my_col * hd, hd), hd)

                @pl.when(dest != me)
                def _():
                    rcopy(onat.at[pl.ds(s_i * seg, seg), :], orecv.at[pl.ds(seg * r, seg), cols_o],
                          osend.at[s_i], orecvs.at[my_col, r], dest).start()

                @pl.when(dest == me)
                def _():
                    orecv[pl.ds(seg * r, seg), cols_o] = onat[s_i * seg:(s_i + 1) * seg, :]

        for j in range(hpc):
            @pl.when(hbase + j != me)
            def _():
                for r in range(2):
                    rcopy(onat.at[pl.ds(0, seg), :], orecv.at[pl.ds(seg * r, seg), pl.ds(hd * j, hd)],
                          osend.at[0], orecvs.at[j, r], hbase + j).wait_recv()

        w_copy(l, 3).wait()
        partial_exchange(lambda cols: dot(orecv[...], bo[:, :, cols].reshape(hpc * hd, ncol)))
        prefetch(3)
        norm_exchange(gm[l], hb)
        w_copy(l, 4).wait()
        w_copy(l, 5).wait()
        fc = 256

        def mlp(i, _):
            cols = pl.ds(al(i * fc, fc), fc)
            g = dot(hb[...], bg[:, cols])
            u = dot(hb[...], bu[:, cols])
            a = (jax.nn.silu(g) * u).astype(BF16)
            cid = lax.broadcasted_iota(jnp.int32, (2 * seg, fc), 1) + i * fc
            act[:, cols] = jnp.where(cid >= core * (fw - foff), a, jnp.zeros_like(a))
            return 0
        lax.fori_loop(0, fw // fc, mlp, 0)
        prefetch(4)
        prefetch(5)
        w_copy(l, 6).wait()
        partial_exchange(lambda cols: dot(act[...], bd[:, cols]))
        prefetch(6)

        for i in range(2):
            cache_copy(i).wait()
        for t in range(3):
            for j in range(hpc):
                @pl.when(hbase + j != me)
                def _():
                    for r in range(2):
                        rcopy(stage.at[t, j, pl.ds(seg * r, seg), :], nat.at[par, t, pl.ds(0, seg), :],
                              qsend.at[t, j, r], qrecv.at[par, t, 0], hbase + j).wait_send()
        for s_i in range(nseg):
            dest = 2 * min(s_i, nseg - 1 - s_i) + src_core

            @pl.when(dest != me)
            def _():
                rcopy(onat.at[pl.ds(s_i * seg, seg), :], orecv.at[pl.ds(0, seg), pl.ds(0, hd)],
                      osend.at[s_i], orecvs.at[0, 0], dest).wait_send()
        return 0

    lax.fori_loop(0, n_layers, layer, 0)
    x_out[...] = xs[...].astype(BF16)


def solution(mesh):
    cp = mesh.shape["cp"]
    row_spec = P(("req", "cp"), None)
    rep = P()
    cache_spec = P(None, "req", "cp", None)

    def per_device(hidden, positions, ga, gm, wq, wk, wv, wo, wg, wu, wd):
        rows, dim = hidden.shape
        n_layers, _, heads, hd = wq.shape
        ff = wg.shape[2]
        seq = rows * cp
        half = rows // 2
        seg = rows
        nseg = seq // seg
        hpc = heads // 2
        tiles = ff // 128
        fw = -(-tiles // 4) * 2 * 128
        foff = ff - fw
        cfg = (cp, n_layers, half, seq, heads, hd, dim, fw, foff)
        cs = rope_tables(positions, hd)
        vm = pl.BlockSpec(memory_space=pltpu.VMEM)
        hb = pl.BlockSpec(memory_space=pltpu.HBM)
        dma = pltpu.SemaphoreType.DMA
        V = pltpu.VMEM
        x, kc, vc = pl.pallas_call(
            functools.partial(kernel, cfg),
            out_shape=(jax.ShapeDtypeStruct((rows, dim), BF16),
                       jax.ShapeDtypeStruct((n_layers, seq, hd), BF16),
                       jax.ShapeDtypeStruct((n_layers, seq, hd), BF16)),
            in_specs=[vm] * 4 + [hb] * 7,
            out_specs=(vm, hb, hb),
            scratch_shapes=[
                V((rows, dim), F32), V((2, 2 * seg, hd), F32), V((2 * seg, dim), BF16), V((2 * seg, dim), BF16),
                V((2 * seg, hpc * hd), F32), V((3, hpc, 2 * seg, hd), BF16), V((2, 3, seq, hd), BF16), V((seq, hd), BF16),
                V((2 * seg, hpc * hd), BF16), V((2 * seg, fw), BF16), V((2 * seg, dim), F32), V((rows, dim), F32), V((8, 128), F32),
                V((3, dim, hpc, hd), BF16), V((hpc, hd, dim), BF16), V((dim, fw), BF16), V((dim, fw), BF16), V((fw, dim), BF16),
                dma((7,)), dma((2,)), dma((2,)), dma((2,)), dma((2,)), dma((2,)), dma((4, 2)), dma((4, 2)),
                dma((3, hpc, 2)), dma((2, 3, nseg)), dma((nseg,)), dma((hpc, 2)),
            ],
            compiler_params=pltpu.CompilerParams(collective_id=0, has_side_effects=True, vmem_limit_bytes=67043328),
            name="prefill",
        )(hidden, cs, ga.reshape(n_layers, 1, dim), gm.reshape(n_layers, 1, dim), wq, wk, wv, wo, wg, wu, wd)
        return x, kc.reshape(n_layers, seq, 1, hd), vc.reshape(n_layers, seq, 1, hd)

    in_specs = (row_spec, P(("req", "cp"))) + (rep,) * 9
    return jax.shard_map(per_device, mesh=mesh, in_specs=in_specs, out_specs=(row_spec, cache_spec, cache_spec), check_vma=False)
```

```python
import functools

import jax
import jax.numpy as jnp
from jax import lax
from jax.experimental import pallas as pl
from jax.experimental.pallas import tpu as pltpu
from jax.sharding import PartitionSpec as P

NORM_EPS = 1e-5
ROPE_BASE = 10000.0
F32 = jnp.float32
BF16 = jnp.bfloat16


def rope_tables(pos_vec, head_dim):
    inv_freq = ROPE_BASE ** (-jnp.arange(0, head_dim, 2, dtype=F32) / head_dim)
    angles = pos_vec.astype(F32)[..., None] * inv_freq
    cos_tab, sin_tab = jnp.cos(angles), jnp.sin(angles)
    return cos_tab, sin_tab


def dot(a, b):
    return jnp.dot(a, b, preferred_element_type=F32)


def kernel(cfg, x_in, cos_in, sin_in, ga, gm, wq, wk, wv, wo, wg, wu, wd, x_out, kc, vc,
           xs, gains, tab, hbuf, act, stage, nat, onat, probs, orecv, pfull, precv,
           bqkv, bo, bg, bu, bd, wsem, csem, isend, irecv, psend, precvs,
           qsend, qrecv, osend, orecvs):
    cp, n_layers, half, seq, heads, hd, dim, fw, foff = cfg
    seg = 2 * half
    nseg = seq // seg
    hpc = heads // 2
    nchip = cp // 2
    me = lax.axis_index("cp")
    core = lax.rem(me, 2)
    chip = me // 2
    partner = me + 1 - 2 * core

    def al(v, m):
        return pl.multiple_of(v, m)

    my_rows = (al(half * core, half), al(seg + half * (1 - core), half))
    pa_rows = (al(half * (1 - core), half), al(seg + half * core, half))
    hbase = al(hpc * lax.rem(core + chip + chip // (nchip // 2), 2), hpc)
    my_half = me // hpc
    my_col = lax.rem(me, hpc)

    def worker(z):
        return 2 * z + lax.rem(my_half + z + z // (nchip // 2), 2)

    def rcopy(src, dst, ss, rs, dev):
        return pltpu.make_async_remote_copy(src_ref=src, dst_ref=dst, send_sem=ss, recv_sem=rs,
                                            device_id={"cp": dev}, device_id_type=pl.DeviceIdType.MESH)

    qkv_hbm = (wk, wq, wv)

    def w_copy(l, i):
        fo = al(core * foff, 128)
        if i < 3:
            src, dst = qkv_hbm[i].at[l, :, pl.ds(hbase, hpc), :], bqkv.at[i]
        elif i == 3:
            src, dst = wo.at[l, pl.ds(hbase, hpc)], bo
        elif i < 6:
            src, dst = (wg, wu)[i - 4].at[l, :, pl.ds(fo, fw)], (bg, bu)[i - 4]
        else:
            src, dst = wd.at[l, pl.ds(fo, fw), :], bd
        return pltpu.make_async_copy(src, dst, wsem.at[i])

    for i in range(7):
        w_copy(0, i).start()

    for i in range(2):
        rows = slice(half * i, half * (i + 1))
        xs[pl.ds(my_rows[i], half), :] = x_in[rows, :]
        cos_t, sin_t = cos_in[rows, :], sin_in[rows, :]
        tab[0, pl.ds(my_rows[i], half), :] = jnp.concatenate([cos_t, cos_t], axis=-1)
        tab[1, pl.ds(my_rows[i], half), :] = jnp.concatenate([-sin_t, sin_t], axis=-1)
    gains[0] = ga[...].astype(F32)
    gains[1] = gm[...].astype(F32)

    barrier = pltpu.get_barrier_semaphore()
    for d in range(1, cp):
        pl.semaphore_signal(barrier, inc=1, device_id={"cp": lax.rem(me + d, cp)}, device_id_type=pl.DeviceIdType.MESH)
    pl.semaphore_wait(barrier, cp - 1)

    def first(rows, i):
        r = pl.ds(rows[i], half)
        return (rcopy(x_in.at[pl.ds(half * i, half), :], xs.at[r, :], isend.at[0, i], irecv.at[0, i], partner),
                rcopy(tab.at[:, r, :], tab.at[:, r, :], isend.at[1, i], irecv.at[1, i], partner))

    for i in range(2):
        for c in first(my_rows, i):
            c.start()
    for i in range(2):
        for c in first(pa_rows, i):
            c.wait_recv()
        for c in first(my_rows, i):
            c.wait_send()

    def norm(which, l):
        xv = xs[...].astype(F32)
        inv = lax.rsqrt(jnp.mean(xv * xv, axis=-1, keepdims=True) + NORM_EPS)
        hbuf[...] = (xv * inv * gains[which, pl.ds(l, 1), :]).astype(BF16)

    def partial_exchange(w, product, widths):
        starts = [sum(widths[:i]) for i in range(len(widths))]

        def pcopy(i):
            cols = pl.ds(starts[i], widths[i])
            return rcopy(pfull.at[:, cols], precv.at[w, :, cols], psend.at[w, i], precvs.at[w, i], partner)

        for i in range(len(widths)):
            cols = slice(starts[i], starts[i] + widths[i])
            pfull[:, cols] = product(cols)
            pcopy(i).start()
        for i in range(len(widths)):
            cols = slice(starts[i], starts[i] + widths[i])
            pcopy(i).wait()
            xs[:, cols] = (xs[:, cols].astype(F32) + (pfull[:, cols] + precv[w, :, cols])).astype(BF16)

    def layer(l, _):
        par = lax.rem(l, 2)

        def prefetch(i):
            @pl.when(l + 1 < n_layers)
            def _():
                w_copy(l + 1, i).start()

        norm(0, l)
        segs = (chip, nseg - 1 - chip)

        def send(t, r):
            for j in range(hpc):
                n = hbase + j
                rows = pl.ds(al(segs[r] * seg, seg), seg)

                @pl.when(n != me)
                def _():
                    rcopy(stage.at[t, j, pl.ds(seg * r, seg), :], nat.at[par, t, rows, :],
                          qsend.at[t, j, r], qrecv.at[par, t, segs[r]], n).start()

                @pl.when(n == me)
                def _():
                    nat[par, t, rows, :] = stage[t, j, seg * r:seg * (r + 1), :]

        for t in range(3):
            w_copy(l, t).wait()
            prod = dot(hbuf[...], bqkv[t].reshape(dim, hpc * hd))
            prefetch(t)
            for j in range(hpc):
                a = prod[:, hd * j:hd * (j + 1)]
                if t < 2:
                    a = a * tab[0] + pltpu.roll(a, hd // 2, 1) * tab[1]
                stage[t, j] = a.astype(BF16)
            send(t, 0)
        for t in range(3):
            send(t, 1)

        def wait_nat(t, r):
            for s in range(r * nseg // 2, (r + 1) * nseg // 2):
                src = worker(min(s, nseg - 1 - s))

                @pl.when(src != me)
                def _():
                    rcopy(stage.at[t, 0, pl.ds(0, seg), :], nat.at[par, t, pl.ds(s * seg, seg), :],
                          qsend.at[t, 0, 0], qrecv.at[par, t, s], src).wait_recv()

        def cache_copy(i):
            return pltpu.make_async_copy(nat.at[par, 2 * i], (kc, vc)[i].at[l], csem.at[i])

        qb = 256
        half_b = seq // qb // 2

        def softmax(b):
            n_keys = qb * (b + 1)
            q = nat[par, 1, pl.ds(qb * b, qb), :]
            k = nat[par, 0, pl.ds(0, n_keys), :]
            s = lax.dot_general(q, k, (((1,), (1,)), ((), ())), preferred_element_type=F32) * (hd ** -0.5)
            rows = lax.broadcasted_iota(jnp.int32, (qb, qb), 0)
            cols = lax.broadcasted_iota(jnp.int32, (qb, qb), 1)
            last = jnp.where(cols <= rows, s[:, n_keys - qb:], -jnp.inf)
            s = last if b == 0 else jnp.concatenate([s[:, :n_keys - qb], last], axis=1)
            e = jnp.exp(s - jnp.max(s, axis=-1, keepdims=True))
            return (e * (1.0 / jnp.sum(e, axis=-1, keepdims=True))).astype(BF16)

        def attend(b, p):
            onat[pl.ds(qb * b, qb), :] = dot(p, nat[par, 2, pl.ds(0, qb * (b + 1)), :]).astype(BF16)
            for s_i in range(b * qb // seg, (b + 1) * qb // seg):
                r = 1 if s_i >= nseg // 2 else 0
                dest = worker(min(s_i, nseg - 1 - s_i))
                cols_o = pl.ds(al(my_col * hd, hd), hd)

                @pl.when(dest != me)
                def _():
                    rcopy(onat.at[pl.ds(s_i * seg, seg), :], orecv.at[pl.ds(seg * r, seg), cols_o],
                          osend.at[s_i], orecvs.at[my_col, r], dest).start()

                @pl.when(dest == me)
                def _():
                    orecv[pl.ds(seg * r, seg), cols_o] = onat[s_i * seg:(s_i + 1) * seg, :]

        for t in range(3):
            wait_nat(t, 0)
        for b in range(half_b):
            attend(b, softmax(b))
        wait_nat(0, 1)
        cache_copy(0).start()
        wait_nat(1, 1)
        for b in range(half_b, 2 * half_b):
            probs[b - half_b, :, :qb * (b + 1)] = softmax(b)
        wait_nat(2, 1)
        cache_copy(1).start()
        for b in range(half_b, 2 * half_b):
            attend(b, probs[b - half_b, :, :qb * (b + 1)])

        for j in range(hpc):
            @pl.when(hbase + j != me)
            def _():
                for r in range(2):
                    rcopy(onat.at[pl.ds(0, seg), :], orecv.at[pl.ds(seg * r, seg), pl.ds(hd * j, hd)],
                          osend.at[0], orecvs.at[j, r], hbase + j).wait_recv()

        w_copy(l, 3).wait()
        partial_exchange(0, lambda cols: dot(orecv[...], bo[:, :, cols].reshape(hpc * hd, cols.stop - cols.start)),
                         (dim // 2, dim // 2))
        prefetch(3)
        norm(1, l)
        w_copy(l, 4).wait()
        w_copy(l, 5).wait()
        fc = fw // 2
        for i in range(2):
            cols = slice(fc * i, fc * (i + 1))
            a = (jax.nn.silu(dot(hbuf[...], bg[:, cols])) * dot(hbuf[...], bu[:, cols])).astype(BF16)
            if i == 0:
                cid = lax.broadcasted_iota(jnp.int32, (2 * seg, fc), 1)
                a = jnp.where(cid >= core * (fw - foff), a, jnp.zeros_like(a))
            act[:, cols] = a
        prefetch(4)
        prefetch(5)
        w_copy(l, 6).wait()
        partial_exchange(1, lambda cols: dot(act[...], bd[:, cols]), (dim // 2, dim // 4, dim // 4))
        prefetch(6)

        for i in range(2):
            cache_copy(i).wait()
        for t in range(3):
            for j in range(hpc):
                @pl.when(hbase + j != me)
                def _():
                    for r in range(2):
                        rcopy(stage.at[t, j, pl.ds(seg * r, seg), :], nat.at[par, t, pl.ds(0, seg), :],
                              qsend.at[t, j, r], qrecv.at[par, t, 0], hbase + j).wait_send()
        for s_i in range(nseg):
            dest = worker(min(s_i, nseg - 1 - s_i))

            @pl.when(dest != me)
            def _():
                rcopy(onat.at[pl.ds(s_i * seg, seg), :], orecv.at[pl.ds(0, seg), pl.ds(0, hd)],
                      osend.at[s_i], orecvs.at[0, 0], dest).wait_send()
        return 0

    lax.fori_loop(0, n_layers, layer, 0)
    for i in range(2):
        x_out[half * i:half * (i + 1), :] = xs[pl.ds(my_rows[i], half), :]


def copy_out(n, *refs):
    srcs, dsts, bufs, sem = refs[:n], refs[n:2 * n], refs[2 * n:3 * n], refs[3 * n]
    ins = [pltpu.make_async_copy(srcs[i], bufs[i], sem.at[0, i]) for i in range(n)]
    outs = [pltpu.make_async_copy(bufs[i], dsts[i], sem.at[1, i]) for i in range(n)]
    for c in ins:
        c.start()
    for i in range(n):
        ins[i].wait()
        outs[i].start()
    for c in outs:
        c.wait()


def solution(mesh):
    cp = mesh.shape["cp"]
    row_spec = P(("req", "cp"), None)
    rep = P()
    cache_spec = P(None, "req", "cp", None)

    def per_device(hidden, positions, ga, gm, wq, wk, wv, wo, wg, wu, wd):
        rows, dim = hidden.shape
        n_layers, _, heads, hd = wq.shape
        ff = wg.shape[2]
        seq = rows * cp
        half = rows // 2
        seg = rows
        nseg = seq // seg
        hpc = heads // 2
        tiles = ff // 128
        fw = -(-tiles // 4) * 2 * 128
        foff = ff - fw
        cfg = (cp, n_layers, half, seq, heads, hd, dim, fw, foff)
        cos_tab, sin_tab = rope_tables(positions, hd)
        vm = pl.BlockSpec(memory_space=pltpu.VMEM)
        hb = pl.BlockSpec(memory_space=pltpu.HBM)
        dma = pltpu.SemaphoreType.DMA
        V = pltpu.VMEM
        outs = (jax.ShapeDtypeStruct((rows, dim), BF16),
                jax.ShapeDtypeStruct((n_layers, seq, hd), BF16),
                jax.ShapeDtypeStruct((n_layers, seq, hd), BF16))
        res = pl.pallas_call(
            functools.partial(kernel, cfg),
            out_shape=outs,
            in_specs=[vm] * 5 + [hb] * 7,
            out_specs=(vm, hb, hb),
            scratch_shapes=[
                V((2 * seg, dim), BF16), V((2, n_layers, dim), F32), V((2, 2 * seg, hd), F32), V((2 * seg, dim), BF16),
                V((2 * seg, fw), BF16), V((3, hpc, 2 * seg, hd), BF16), V((2, 3, seq, hd), BF16), V((seq, hd), BF16),
                V((2, 256, seq), BF16), V((2 * seg, hpc * hd), BF16), V((2 * seg, dim), F32), V((2, 2 * seg, dim), F32),
                V((3, dim, hpc, hd), BF16), V((hpc, hd, dim), BF16), V((dim, fw), BF16), V((dim, fw), BF16), V((fw, dim), BF16),
                dma((7,)), dma((2,)), dma((2, 2)), dma((2, 2)), dma((2, 3)), dma((2, 3)),
                dma((3, hpc, 2)), dma((2, 3, nseg)), dma((nseg,)), dma((hpc, 2)),
            ],
            compiler_params=pltpu.CompilerParams(collective_id=0, has_side_effects=True, vmem_limit_bytes=67043328),
            name="prefill",
        )(hidden, cos_tab, sin_tab, ga, gm, wq, wk, wv, wo, wg, wu, wd)
        x, kc, vc = pl.pallas_call(
            functools.partial(copy_out, 3), out_shape=outs, in_specs=[hb] * 3, out_specs=(hb,) * 3,
            scratch_shapes=[V(o.shape, o.dtype) for o in outs] + [dma((2, 3))], name="copy_out",
        )(*res)
        return x, kc.reshape(n_layers, seq, 1, hd), vc.reshape(n_layers, seq, 1, hd)

    in_specs = (row_spec, P(("req", "cp"))) + (rep,) * 9
    return jax.shard_map(per_device, mesh=mesh, in_specs=in_specs, out_specs=(row_spec, cache_spec, cache_spec), check_vma=False)
```

```python
import functools

import jax
import jax.numpy as jnp
from jax import lax
from jax.experimental import pallas as pl
from jax.experimental.pallas import tpu as pltpu
from jax.sharding import PartitionSpec as P

NORM_EPS = 1e-5
ROPE_BASE = 10000.0
F32 = jnp.float32
BF16 = jnp.bfloat16


def rope_tables(pos_vec, head_dim):
    inv_freq = ROPE_BASE ** (-jnp.arange(0, head_dim, 2, dtype=F32) / head_dim)
    angles = pos_vec.astype(F32)[..., None] * inv_freq
    cos_tab, sin_tab = jnp.cos(angles), jnp.sin(angles)
    return cos_tab, sin_tab


def dot(a, b):
    return jnp.dot(a, b, preferred_element_type=F32)


def kernel(cfg, x_in, cos_in, sin_in, ga, gm, wq, wk, wv, wo, wg, wu, wd, x_out, kc, vc,
           xs, gains, tab, hbuf, act, stage, nat, onat, probs, orecv, pfull, precv,
           bqkv, bo, bg, bu, bd, wsem, csem, isend, irecv, psend, precvs,
           qsend, qrecv, osend, orecvs):
    cp, n_layers, half, seq, heads, hd, dim, fw, foff = cfg
    seg = 2 * half
    nseg = seq // seg
    hpc = heads // 2
    nchip = cp // 2
    me = lax.axis_index("cp")
    core = lax.rem(me, 2)
    chip = me // 2
    partner = me + 1 - 2 * core

    def al(v, m):
        return pl.multiple_of(v, m)

    my_rows = (al(half * core, half), al(seg + half * (1 - core), half))
    pa_rows = (al(half * (1 - core), half), al(seg + half * core, half))
    hbase = al(hpc * lax.rem(core + chip + chip // (nchip // 2), 2), hpc)
    my_half = me // hpc
    my_col = lax.rem(me, hpc)

    def worker(z):
        return 2 * z + lax.rem(my_half + z + z // (nchip // 2), 2)

    def rcopy(src, dst, ss, rs, dev):
        return pltpu.make_async_remote_copy(src_ref=src, dst_ref=dst, send_sem=ss, recv_sem=rs,
                                            device_id={"cp": dev}, device_id_type=pl.DeviceIdType.MESH)

    qkv_hbm = (wk, wq, wv)

    def w_copy(l, i):
        fo = al(core * foff, 128)
        if i < 3:
            src, dst = qkv_hbm[i].at[l, :, pl.ds(hbase, hpc), :], bqkv.at[i]
        elif i == 3:
            src, dst = wo.at[l, pl.ds(hbase, hpc)], bo
        elif i < 6:
            src, dst = (wg, wu)[i - 4].at[l, :, pl.ds(fo, fw)], (bg, bu)[i - 4]
        else:
            src, dst = wd.at[l, pl.ds(fo, fw), :], bd
        return pltpu.make_async_copy(src, dst, wsem.at[i])

    for i in range(7):
        w_copy(0, i).start()

    for i in range(2):
        rows = slice(half * i, half * (i + 1))
        xs[pl.ds(my_rows[i], half), :] = x_in[rows, :]
        cos_t, sin_t = cos_in[rows, :], sin_in[rows, :]
        tab[0, pl.ds(my_rows[i], half), :] = jnp.concatenate([cos_t, cos_t], axis=-1)
        tab[1, pl.ds(my_rows[i], half), :] = jnp.concatenate([-sin_t, sin_t], axis=-1)
    gains[0] = ga[...].astype(F32)
    gains[1] = gm[...].astype(F32)

    barrier = pltpu.get_barrier_semaphore()
    for d in range(1, cp):
        pl.semaphore_signal(barrier, inc=1, device_id={"cp": lax.rem(me + d, cp)}, device_id_type=pl.DeviceIdType.MESH)
    pl.semaphore_wait(barrier, cp - 1)

    def first(rows, i):
        r = pl.ds(rows[i], half)
        return (rcopy(x_in.at[pl.ds(half * i, half), :], xs.at[r, :], isend.at[0, i], irecv.at[0, i], partner),
                rcopy(tab.at[:, r, :], tab.at[:, r, :], isend.at[1, i], irecv.at[1, i], partner))

    for i in range(2):
        for c in first(my_rows, i):
            c.start()
    for i in range(2):
        for c in first(pa_rows, i):
            c.wait_recv()
        for c in first(my_rows, i):
            c.wait_send()

    is_self = lax.rem(core + chip + chip // (nchip // 2), 2) == my_half

    def wait_all(recv, sem):
        def go(count):
            ref = nat.at[0, 0, pl.ds(0, count * seg), :]
            c = rcopy(ref, ref, sem, sem, partner)
            if recv:
                c.wait_recv()
            else:
                c.wait_send()

        @pl.when(is_self)
        def _():
            go(nchip - 1)

        @pl.when(jnp.logical_not(is_self))
        def _():
            go(nchip)

    def half_rows(r):
        return pl.ds(al(seg * r, seg), seg)

    def norm(which, l, r):
        rows = half_rows(r)
        xv = xs[rows, :].astype(F32)
        inv = lax.rsqrt(jnp.mean(xv * xv, axis=-1, keepdims=True) + NORM_EPS)
        hbuf[rows, :] = (xv * inv * gains[which, pl.ds(l, 1), :]).astype(BF16)

    def chunks(widths):
        starts = [sum(widths[:i]) for i in range(len(widths))]
        return [slice(c, c + w) for c, w in zip(starts, widths)]

    def pcopy(w, r, i, cols):
        rows, cs = half_rows(r), pl.ds(cols.start, cols.stop - cols.start)
        return rcopy(pfull.at[rows, cs], precv.at[w, rows, cs], psend.at[w, r, i], precvs.at[w, r, i], partner)

    def partial_start(w, r, product, widths):
        for i, cols in enumerate(chunks(widths)):
            pfull[half_rows(r), cols] = product(cols)
            pcopy(w, r, i, cols).start()

    def partial_finish(w, r, widths):
        rows = half_rows(r)
        for i, cols in enumerate(chunks(widths)):
            pcopy(w, r, i, cols).wait()
            xs[rows, cols] = (xs[rows, cols].astype(F32) + (pfull[rows, cols] + precv[w, rows, cols])).astype(BF16)

    def w_wait(l, r, i):
        @pl.when(r == 0)
        def _():
            w_copy(l, i).wait()

    def prefetch(l, r, i):
        @pl.when((r == 1) & (l + 1 < n_layers))
        def _():
            w_copy(l + 1, i).start()

    wo_widths = (dim // 2, dim // 2)
    wd_widths = (dim // 2, dim // 4, dim // 4)
    qb = 256
    half_b = seq // qb // 2

    def qkv(l, r):
        par = lax.rem(l, 2)
        hrows = half_rows(r)
        norm(0, l, r)
        seg_id = chip + r * (nseg - 1 - 2 * chip)
        for t in range(3):
            w_wait(l, r, t)
            prod = dot(hbuf[hrows, :], bqkv[t].reshape(dim, hpc * hd))
            prefetch(l, r, t)
            for j in range(hpc):
                a = prod[:, hd * j:hd * (j + 1)]
                if t < 2:
                    a = a * tab[0, hrows, :] + pltpu.roll(a, hd // 2, 1) * tab[1, hrows, :]
                stage[t, j, hrows, :] = a.astype(BF16)
            rows = pl.ds(al(seg_id * seg, seg), seg)
            for j in range(hpc):
                n = hbase + j

                @pl.when(n != me)
                def _():
                    rcopy(stage.at[t, j, hrows, :], nat.at[par, t, rows, :],
                          qsend.at[t, r], qrecv.at[par, t, r], n).start()

                @pl.when(n == me)
                def _():
                    nat[par, t, rows, :] = stage[t, j, hrows, :]

    def attention(l, r):
        par = lax.rem(l, 2)

        def softmax(b):
            n_keys = qb * (b + 1)
            q = nat[par, 1, pl.ds(qb * b, qb), :]
            k = nat[par, 0, pl.ds(0, n_keys), :]
            s = lax.dot_general(q, k, (((1,), (1,)), ((), ())), preferred_element_type=F32) * (hd ** -0.5)
            rows = lax.broadcasted_iota(jnp.int32, (qb, qb), 0)
            cols = lax.broadcasted_iota(jnp.int32, (qb, qb), 1)
            last = jnp.where(cols <= rows, s[:, n_keys - qb:], -jnp.inf)
            s = last if b == 0 else jnp.concatenate([s[:, :n_keys - qb], last], axis=1)
            e = jnp.exp(s - jnp.max(s, axis=-1, keepdims=True))
            return (e * (1.0 / jnp.sum(e, axis=-1, keepdims=True))).astype(BF16)

        def attend(b, p):
            onat[pl.ds(qb * b, qb), :] = dot(p, nat[par, 2, pl.ds(0, qb * (b + 1)), :]).astype(BF16)
            for s_i in range(b * qb // seg, (b + 1) * qb // seg):
                dest = worker(min(s_i, nseg - 1 - s_i))
                cols_o = pl.ds(al(my_col * hd, hd), hd)

                @pl.when(dest != me)
                def _():
                    rcopy(onat.at[pl.ds(s_i * seg, seg), :], orecv.at[pl.ds(seg * r, seg), cols_o],
                          osend.at[r], orecvs.at[r], dest).start()

                @pl.when(dest == me)
                def _():
                    orecv[pl.ds(seg * r, seg), cols_o] = onat[s_i * seg:(s_i + 1) * seg, :]

        if r == 0:
            for t in range(3):
                wait_all(True, qrecv.at[par, t, 0])
            for b in range(half_b):
                attend(b, softmax(b))
        else:
            wait_all(True, qrecv.at[par, 0, 1])
            cache_copy(l, 0).start()
            wait_all(True, qrecv.at[par, 1, 1])
            for b in range(half_b, 2 * half_b):
                probs[b - half_b, :, :qb * (b + 1)] = softmax(b)
            wait_all(True, qrecv.at[par, 2, 1])
            cache_copy(l, 1).start()
            for b in range(half_b, 2 * half_b):
                attend(b, probs[b - half_b, :, :qb * (b + 1)])

    def cache_copy(l, i):
        return pltpu.make_async_copy(nat.at[lax.rem(l, 2), 2 * i], (kc, vc)[i].at[l], csem.at[i])

    def post(l, r):
        hrows = half_rows(r)
        wait_all(True, orecvs.at[r])
        w_wait(l, r, 3)
        partial_start(0, r, lambda cols: dot(orecv[hrows, :], bo[:, :, cols].reshape(hpc * hd, cols.stop - cols.start)), wo_widths)
        prefetch(l, r, 3)
        for t in range(3):
            wait_all(False, qsend.at[t, r])
        wait_all(False, osend.at[r])
        partial_finish(0, r, wo_widths)
        norm(1, l, r)
        w_wait(l, r, 4)
        w_wait(l, r, 5)
        fc = fw // 2
        for i in range(2):
            cols = slice(fc * i, fc * (i + 1))
            a = (jax.nn.silu(dot(hbuf[hrows, :], bg[:, cols])) * dot(hbuf[hrows, :], bu[:, cols])).astype(BF16)
            if i == 0:
                cid = lax.broadcasted_iota(jnp.int32, (seg, fc), 1)
                a = jnp.where(cid >= core * (fw - foff), a, jnp.zeros_like(a))
            act[hrows, cols] = a
        prefetch(l, r, 4)
        prefetch(l, r, 5)
        w_wait(l, r, 6)
        partial_start(1, r, lambda cols: dot(act[hrows, :], bd[:, cols]), wd_widths)
        prefetch(l, r, 6)

    def step(i, _):
        l_now, r_now = (i + 1) // 2 - 1, lax.rem(i + 1, 2)
        r_next = lax.rem(i, 2)
        for r in range(2):
            @pl.when((i > 0) & (r_now == r))
            def _():
                attention(l_now, r)

        @pl.when(i > 1)
        def _():
            partial_finish(1, r_next, wd_widths)

        @pl.when(i < 2 * n_layers)
        def _():
            qkv(i // 2, r_next)

        @pl.when(i > 0)
        def _():
            post(l_now, r_now)

        @pl.when((i > 0) & (r_now == 1))
        def _():
            for c in range(2):
                cache_copy(l_now, c).wait()
        return 0

    lax.fori_loop(0, 2 * n_layers + 1, step, 0)
    partial_finish(1, 1, wd_widths)
    for i in range(2):
        x_out[half * i:half * (i + 1), :] = xs[pl.ds(my_rows[i], half), :]


def copy_out(n, *refs):
    srcs, dsts, bufs, sem = refs[:n], refs[n:2 * n], refs[2 * n:3 * n], refs[3 * n]
    ins = [pltpu.make_async_copy(srcs[i], bufs[i], sem.at[0, i]) for i in range(n)]
    outs = [pltpu.make_async_copy(bufs[i], dsts[i], sem.at[1, i]) for i in range(n)]
    for c in ins:
        c.start()
    for i in range(n):
        ins[i].wait()
        outs[i].start()
    for c in outs:
        c.wait()


def solution(mesh):
    cp = mesh.shape["cp"]
    row_spec = P(("req", "cp"), None)
    rep = P()
    cache_spec = P(None, "req", "cp", None)

    def per_device(hidden, positions, ga, gm, wq, wk, wv, wo, wg, wu, wd):
        rows, dim = hidden.shape
        n_layers, _, heads, hd = wq.shape
        ff = wg.shape[2]
        seq = rows * cp
        half = rows // 2
        seg = rows
        nseg = seq // seg
        hpc = heads // 2
        tiles = ff // 128
        fw = -(-tiles // 4) * 2 * 128
        foff = ff - fw
        cfg = (cp, n_layers, half, seq, heads, hd, dim, fw, foff)
        cos_tab, sin_tab = rope_tables(positions, hd)
        vm = pl.BlockSpec(memory_space=pltpu.VMEM)
        hb = pl.BlockSpec(memory_space=pltpu.HBM)
        dma = pltpu.SemaphoreType.DMA
        V = pltpu.VMEM
        outs = (jax.ShapeDtypeStruct((rows, dim), BF16),
                jax.ShapeDtypeStruct((n_layers, seq, hd), BF16),
                jax.ShapeDtypeStruct((n_layers, seq, hd), BF16))
        res = pl.pallas_call(
            functools.partial(kernel, cfg),
            out_shape=outs,
            in_specs=[vm] * 5 + [hb] * 7,
            out_specs=(vm, hb, hb),
            scratch_shapes=[
                V((2 * seg, dim), BF16), V((2, n_layers, dim), F32), V((2, 2 * seg, hd), F32), V((2 * seg, dim), BF16),
                V((2 * seg, fw), BF16), V((3, hpc, 2 * seg, hd), BF16), V((2, 3, seq, hd), BF16), V((seq, hd), BF16),
                V((2, 256, seq), BF16), V((2 * seg, hpc * hd), BF16), V((2 * seg, dim), F32), V((2, 2 * seg, dim), F32),
                V((3, dim, hpc, hd), BF16), V((hpc, hd, dim), BF16), V((dim, fw), BF16), V((dim, fw), BF16), V((fw, dim), BF16),
                dma((7,)), dma((2,)), dma((2, 2)), dma((2, 2)), dma((2, 2, 3)), dma((2, 2, 3)),
                dma((3, 2)), dma((2, 3, 2)), dma((2,)), dma((2,)),
            ],
            compiler_params=pltpu.CompilerParams(collective_id=0, has_side_effects=True, vmem_limit_bytes=67043328),
            name="prefill",
        )(hidden, cos_tab, sin_tab, ga, gm, wq, wk, wv, wo, wg, wu, wd)
        x, kc, vc = pl.pallas_call(
            functools.partial(copy_out, 3), out_shape=outs, in_specs=[hb] * 3, out_specs=(hb,) * 3,
            scratch_shapes=[V(o.shape, o.dtype) for o in outs] + [dma((2, 3))], name="copy_out",
        )(*res)
        return x, kc.reshape(n_layers, seq, 1, hd), vc.reshape(n_layers, seq, 1, hd)

    in_specs = (row_spec, P(("req", "cp"))) + (rep,) * 9
    return jax.shard_map(per_device, mesh=mesh, in_specs=in_specs, out_specs=(row_spec, cache_spec, cache_spec), check_vma=False)
```

```python
import functools

import jax
import jax.numpy as jnp
from jax import lax
from jax.experimental import pallas as pl
from jax.experimental.pallas import tpu as pltpu
from jax.sharding import PartitionSpec as P

NORM_EPS = 1e-5
ROPE_BASE = 10000.0
F32 = jnp.float32
BF16 = jnp.bfloat16


def rope_tables(pos_vec, head_dim):
    inv_freq = ROPE_BASE ** (-jnp.arange(0, head_dim, 2, dtype=F32) / head_dim)
    angles = pos_vec.astype(F32)[..., None] * inv_freq
    cos_tab, sin_tab = jnp.cos(angles), jnp.sin(angles)
    return cos_tab, sin_tab


def dot(a, b):
    return jnp.dot(a, b, preferred_element_type=F32)


def kernel(cfg, x_in, cos_in, sin_in, ga, gm, wq, wk, wv, wo, wg, wu, wd, x_out, kc, vc,
           xs, gains, tab, hbuf, act, stage, nat, onat, probs, orecv, pfull, precv,
           bqkv, bo, bg, bu, bd, wsem, csem, isend, irecv, psend, precvs,
           qsend, qrecv, osend, orecvs):
    cp, n_layers, half, seq, heads, hd, dim, fw, foff = cfg
    seg = 2 * half
    nseg = seq // seg
    hpc = heads // 2
    nchip = cp // 2
    me = lax.axis_index("cp")
    core = lax.rem(me, 2)
    chip = me // 2
    partner = me + 1 - 2 * core

    def al(v, m):
        return pl.multiple_of(v, m)

    my_rows = (al(half * core, half), al(seg + half * (1 - core), half))
    pa_rows = (al(half * (1 - core), half), al(seg + half * core, half))
    hbase = al(hpc * lax.rem(core + chip + chip // (nchip // 2), 2), hpc)
    my_half = me // hpc
    my_col = lax.rem(me, hpc)

    def worker(z):
        return 2 * z + lax.rem(my_half + z + z // (nchip // 2), 2)

    def rcopy(src, dst, ss, rs, dev):
        return pltpu.make_async_remote_copy(src_ref=src, dst_ref=dst, send_sem=ss, recv_sem=rs,
                                            device_id={"cp": dev}, device_id_type=pl.DeviceIdType.MESH)

    qkv_hbm = (wk, wq, wv)

    def w_copy(l, i):
        fo = al(core * foff, 128)
        if i < 3:
            src, dst = qkv_hbm[i].at[l, :, pl.ds(hbase, hpc), :], bqkv.at[i]
        elif i == 3:
            src, dst = wo.at[l, pl.ds(hbase, hpc)], bo
        elif i < 6:
            src, dst = (wg, wu)[i - 4].at[l, :, pl.ds(fo, fw)], (bg, bu)[i - 4]
        else:
            src, dst = wd.at[l, pl.ds(fo, fw), :], bd
        return pltpu.make_async_copy(src, dst, wsem.at[i])

    for i in range(7):
        w_copy(0, i).start()

    for i in range(2):
        rows = slice(half * i, half * (i + 1))
        xs[pl.ds(my_rows[i], half), :] = x_in[rows, :]
        cos_t, sin_t = cos_in[rows, :], sin_in[rows, :]
        tab[0, pl.ds(my_rows[i], half), :] = jnp.concatenate([cos_t, cos_t], axis=-1)
        tab[1, pl.ds(my_rows[i], half), :] = jnp.concatenate([-sin_t, sin_t], axis=-1)
    gains[0] = ga[...].astype(F32)
    gains[1] = gm[...].astype(F32)
    hbuf[...] = jnp.zeros_like(hbuf)

    barrier = pltpu.get_barrier_semaphore()
    for d in range(1, cp):
        pl.semaphore_signal(barrier, inc=1, device_id={"cp": lax.rem(me + d, cp)}, device_id_type=pl.DeviceIdType.MESH)
    pl.semaphore_wait(barrier, cp - 1)

    def first(rows, i):
        r = pl.ds(rows[i], half)
        return (rcopy(x_in.at[pl.ds(half * i, half), :], xs.at[r, :], isend.at[0, i], irecv.at[0, i], partner),
                rcopy(tab.at[:, r, :], tab.at[:, r, :], isend.at[1, i], irecv.at[1, i], partner))

    for i in range(2):
        for c in first(my_rows, i):
            c.start()
    for i in range(2):
        for c in first(pa_rows, i):
            c.wait_recv()
        for c in first(my_rows, i):
            c.wait_send()

    is_self = lax.rem(core + chip + chip // (nchip // 2), 2) == my_half

    def wait_all(recv, sem):
        def go(count):
            ref = nat.at[0, 0, pl.ds(0, count * seg), :]
            c = rcopy(ref, ref, sem, sem, partner)
            if recv:
                c.wait_recv()
            else:
                c.wait_send()

        @pl.when(is_self)
        def _():
            go(nchip - 1)

        @pl.when(jnp.logical_not(is_self))
        def _():
            go(nchip)

    def half_rows(r):
        return pl.ds(al(seg * r, seg), seg)

    def norm(which, l, r):
        rows = half_rows(r)
        xv = xs[rows, :].astype(F32)
        inv = lax.rsqrt(jnp.mean(xv * xv, axis=-1, keepdims=True) + NORM_EPS)
        hbuf[rows, :] = (xv * inv * gains[which, pl.ds(l, 1), :]).astype(BF16)

    def chunks(widths):
        starts = [sum(widths[:i]) for i in range(len(widths))]
        return [slice(c, c + w) for c, w in zip(starts, widths)]

    def pcopy(w, r, i, cols):
        rows, cs = half_rows(r), pl.ds(cols.start, cols.stop - cols.start)
        return rcopy(pfull.at[rows, cs], precv.at[w, rows, cs], psend.at[w, r, i], precvs.at[w, r, i], partner)

    def partial_start(w, r, rows, product, widths):
        for i, cols in enumerate(chunks(widths)):
            pfull[rows, cols] = product(cols)
            pcopy(w, r, i, cols).start()

    def partial_finish(w, r, widths):
        rows = half_rows(r)
        for i, cols in enumerate(chunks(widths)):
            pcopy(w, r, i, cols).wait()
            xs[rows, cols] = (xs[rows, cols].astype(F32) + (pfull[rows, cols] + precv[w, rows, cols])).astype(BF16)

    def w_wait(l, r, i):
        @pl.when(r == 0)
        def _():
            w_copy(l, i).wait()

    def prefetch(l, r, i):
        @pl.when((r == 1) & (l + 1 < n_layers))
        def _():
            w_copy(l + 1, i).start()

    wo_widths = (dim // 2, dim // 2)
    wd_widths = (dim // 2, dim // 4, dim // 4)
    qb = 256
    half_b = seq // qb // 2

    def qkv(l, r):
        par = lax.rem(l, 2)
        hrows = half_rows(r)
        norm(0, l, r)
        seg_id = chip + r * (nseg - 1 - 2 * chip)
        for t in range(3):
            w_wait(l, r, t)
            prod = dot(hbuf[hrows, :], bqkv[t].reshape(dim, hpc * hd))
            prefetch(l, r, t)
            for j in range(hpc):
                a = prod[:, hd * j:hd * (j + 1)]
                if t < 2:
                    a = a * tab[0, hrows, :] + pltpu.roll(a, hd // 2, 1) * tab[1, hrows, :]
                stage[t, j, hrows, :] = a.astype(BF16)
            rows = pl.ds(al(seg_id * seg, seg), seg)
            for d in range(hpc):
                j = lax.rem(my_col + 1 + d, hpc)

                def go():
                    rcopy(stage.at[t, j, hrows, :], nat.at[par, t, rows, :],
                          qsend.at[t, r], qrecv.at[par, t, r], hbase + j).start()

                if d < hpc - 1:
                    go()
                else:
                    pl.when(jnp.logical_not(is_self))(go)

                    @pl.when(is_self)
                    def _():
                        nat[par, t, rows, :] = stage[t, j, hrows, :]

    def attention(l, r):
        par = lax.rem(l, 2)

        def softmax(b):
            n_keys = qb * (b + 1)
            q = nat[par, 1, pl.ds(qb * b, qb), :]
            k = nat[par, 0, pl.ds(0, n_keys), :]
            s = lax.dot_general(q, k, (((1,), (1,)), ((), ())), preferred_element_type=F32) * (hd ** -0.5)
            rows = lax.broadcasted_iota(jnp.int32, (qb, qb), 0)
            cols = lax.broadcasted_iota(jnp.int32, (qb, qb), 1)
            last = jnp.where(cols <= rows, s[:, n_keys - qb:], -jnp.inf)
            s = last if b == 0 else jnp.concatenate([s[:, :n_keys - qb], last], axis=1)
            e = jnp.exp(s - jnp.max(s, axis=-1, keepdims=True))
            return (e * (1.0 / jnp.sum(e, axis=-1, keepdims=True))).astype(BF16)

        def attend(b, p):
            onat[pl.ds(qb * b, qb), :] = dot(p, nat[par, 2, pl.ds(0, qb * (b + 1)), :]).astype(BF16)
            for s_i in range(b * qb // seg, (b + 1) * qb // seg):
                dest = worker(min(s_i, nseg - 1 - s_i))
                cols_o = pl.ds(al(my_col * hd, hd), hd)

                @pl.when(dest != me)
                def _():
                    rcopy(onat.at[pl.ds(s_i * seg, seg), :], orecv.at[pl.ds(seg * r, seg), cols_o],
                          osend.at[r], orecvs.at[r], dest).start()

                @pl.when(dest == me)
                def _():
                    orecv[pl.ds(seg * r, seg), cols_o] = onat[s_i * seg:(s_i + 1) * seg, :]

        if r == 0:
            for t in range(3):
                wait_all(True, qrecv.at[par, t, 0])
            for b in range(half_b):
                attend(b, softmax(b))
        else:
            wait_all(True, qrecv.at[par, 0, 1])
            cache_copy(l, 0).start()
            wait_all(True, qrecv.at[par, 1, 1])
            for b in range(half_b, 2 * half_b):
                probs[b - half_b, :, :qb * (b + 1)] = softmax(b)
            wait_all(True, qrecv.at[par, 2, 1])
            cache_copy(l, 1).start()
            for b in range(half_b, 2 * half_b):
                attend(b, probs[b - half_b, :, :qb * (b + 1)])

    def cache_copy(l, i):
        return pltpu.make_async_copy(nat.at[lax.rem(l, 2), 2 * i], (kc, vc)[i].at[l], csem.at[i])

    def post(l, r):
        hrows = half_rows(r)
        wait_all(True, orecvs.at[r])
        w_wait(l, r, 3)
        partial_start(0, r, hrows, lambda cols: dot(orecv[hrows, :], bo[:, :, cols].reshape(hpc * hd, cols.stop - cols.start)), wo_widths)
        prefetch(l, r, 3)
        for t in range(3):
            wait_all(False, qsend.at[t, r])
        wait_all(False, osend.at[r])
        partial_finish(0, r, wo_widths)
        norm(1, l, r)
        w_wait(l, r, 4)
        w_wait(l, r, 5)
        fc = fw // 2
        for i in range(2):
            cols = slice(fc * i, fc * (i + 1))
            a = (jax.nn.silu(dot(hbuf[...], bg[:, cols])) * dot(hbuf[...], bu[:, cols])).astype(BF16)
            if i == 0:
                cid = lax.broadcasted_iota(jnp.int32, (2 * seg, fc), 1)
                a = jnp.where(cid >= core * (fw - foff), a, jnp.zeros_like(a))
            act[:, cols] = a
        prefetch(l, r, 4)
        prefetch(l, r, 5)
        w_wait(l, r, 6)
        partial_start(1, r, slice(None), lambda cols: dot(act[...], bd[:, cols]), wd_widths)
        prefetch(l, r, 6)

    def step(i, _):
        l_now, r_now = (i + 1) // 2 - 1, lax.rem(i + 1, 2)
        r_next = lax.rem(i, 2)
        for r in range(2):
            @pl.when((i > 0) & (r_now == r))
            def _():
                attention(l_now, r)

        @pl.when(i > 1)
        def _():
            partial_finish(1, r_next, wd_widths)

        @pl.when(i < 2 * n_layers)
        def _():
            qkv(i // 2, r_next)

        @pl.when(i > 0)
        def _():
            post(l_now, r_now)

        @pl.when((i > 0) & (r_now == 1))
        def _():
            for c in range(2):
                cache_copy(l_now, c).wait()
        return 0

    lax.fori_loop(0, 2 * n_layers + 1, step, 0)
    partial_finish(1, 1, wd_widths)
    for i in range(2):
        x_out[half * i:half * (i + 1), :] = xs[pl.ds(my_rows[i], half), :]


def copy_out(n, *refs):
    srcs, dsts, bufs, sem = refs[:n], refs[n:2 * n], refs[2 * n:3 * n], refs[3 * n]
    ins = [pltpu.make_async_copy(srcs[i], bufs[i], sem.at[0, i]) for i in range(n)]
    outs = [pltpu.make_async_copy(bufs[i], dsts[i], sem.at[1, i]) for i in range(n)]
    for c in ins:
        c.start()
    for i in range(n):
        ins[i].wait()
        outs[i].start()
    for c in outs:
        c.wait()


def solution(mesh):
    cp = mesh.shape["cp"]
    row_spec = P(("req", "cp"), None)
    rep = P()
    cache_spec = P(None, "req", "cp", None)

    def per_device(hidden, positions, ga, gm, wq, wk, wv, wo, wg, wu, wd):
        rows, dim = hidden.shape
        n_layers, _, heads, hd = wq.shape
        ff = wg.shape[2]
        seq = rows * cp
        half = rows // 2
        seg = rows
        nseg = seq // seg
        hpc = heads // 2
        tiles = ff // 128
        fw = -(-tiles // 4) * 2 * 128
        foff = ff - fw
        cfg = (cp, n_layers, half, seq, heads, hd, dim, fw, foff)
        cos_tab, sin_tab = rope_tables(positions, hd)
        vm = pl.BlockSpec(memory_space=pltpu.VMEM)
        hb = pl.BlockSpec(memory_space=pltpu.HBM)
        dma = pltpu.SemaphoreType.DMA
        V = pltpu.VMEM
        outs = (jax.ShapeDtypeStruct((rows, dim), BF16),
                jax.ShapeDtypeStruct((n_layers, seq, hd), BF16),
                jax.ShapeDtypeStruct((n_layers, seq, hd), BF16))
        res = pl.pallas_call(
            functools.partial(kernel, cfg),
            out_shape=outs,
            in_specs=[vm] * 5 + [hb] * 7,
            out_specs=(vm, hb, hb),
            scratch_shapes=[
                V((2 * seg, dim), BF16), V((2, n_layers, dim), F32), V((2, 2 * seg, hd), F32), V((2 * seg, dim), BF16),
                V((2 * seg, fw), BF16), V((3, hpc, 2 * seg, hd), BF16), V((2, 3, seq, hd), BF16), V((seq, hd), BF16),
                V((2, 256, seq), BF16), V((2 * seg, hpc * hd), BF16), V((2 * seg, dim), F32), V((2, 2 * seg, dim), F32),
                V((3, dim, hpc, hd), BF16), V((hpc, hd, dim), BF16), V((dim, fw), BF16), V((dim, fw), BF16), V((fw, dim), BF16),
                dma((7,)), dma((2,)), dma((2, 2)), dma((2, 2)), dma((2, 2, 3)), dma((2, 2, 3)),
                dma((3, 2)), dma((2, 3, 2)), dma((2,)), dma((2,)),
            ],
            compiler_params=pltpu.CompilerParams(collective_id=0, has_side_effects=True, vmem_limit_bytes=67043328),
            name="prefill",
        )(hidden, cos_tab, sin_tab, ga, gm, wq, wk, wv, wo, wg, wu, wd)
        x, kc, vc = pl.pallas_call(
            functools.partial(copy_out, 3), out_shape=outs, in_specs=[hb] * 3, out_specs=(hb,) * 3,
            scratch_shapes=[V(o.shape, o.dtype) for o in outs] + [dma((2, 3))], name="copy_out",
        )(*res)
        return x, kc.reshape(n_layers, seq, 1, hd), vc.reshape(n_layers, seq, 1, hd)

    in_specs = (row_spec, P(("req", "cp"))) + (rep,) * 9
    return jax.shard_map(per_device, mesh=mesh, in_specs=in_specs, out_specs=(row_spec, cache_spec, cache_spec), check_vma=False)
```
